32 devices in a mesh: gx: 4 (over y, x), gy: 8 (over z, core).
Axes of the slice: x: 2, y: 2, z: 4, core: 2. Of those that a mesh axis runs over, the one named last changes fastest.
Arguments:
- beam_states: bfloat16 [32, 16384], P('gy', 'gx'), may hold values from -6 to 6
- step_tokens: bfloat16 [2, 32, 16384], P(None, 'gy', 'gx'), may hold values from -6 to 6
- norm_gain: bfloat16 [16384], P('gx'), may hold values from 0.25 to 1.75
- w_gate: bfloat16 [16384, 28672], P('gx', 'gy'), may hold values from -0.046875 to 0.046875
- w_up: bfloat16 [16384, 28672], P('gx', 'gy'), may hold values from -0.046875 to 0.046875
- w_down: bfloat16 [28672, 16384], P('gy', 'gx'), may hold values from -0.03125 to 0.03125
- prompt_table: bfloat16 [256, 16384], P(None, 'gx'), may hold values from -6 to 6
- kept_beams: int32 [8], replicated, may hold values from 0 to 31, as said below
- prompt_ids: int32 [8, 16], replicated, may hold values from 0 to 255
Outputs:
- decoded: bfloat16 [32, 16384], P('gy', 'gx')
- evaluated: bfloat16 [128, 16384], P('gy', 'gx')
The draws below stay inside these ranges and needn't reach their ends.
Inputs may be any that keep to these rules, and one draw needn't show every extreme that they name: `kept_beams`: distinct beam indices.
All inputs are finite; a program needn't handle non-finite values.
Results may differ from the reference program's by a relative error of at most 0.014.
Values may be sent and summed in bfloat16 or wider, within the bound.
No kernel may reach another device: no remote copies, remote signals or barrier semaphores. Data moves between devices by JAX's collectives and lax.ppermute only.
A program may use at most 192 MiB of HBM per device.

```python
import jax
import jax.numpy as jnp
from jax import lax

D = 16384
FF = 28672
KEPT = 8
PROMPT = 16
PTOK = 256
STEPS = 2
BEAMS = 32


def draw_kept_beams(key, part):
    inner = 1 + jax.random.permutation(jax.random.fold_in(key, 11), BEAMS - 2)[:KEPT - 2]
    ends = jnp.array([0, BEAMS - 1], dtype=jnp.int32)
    whole = jnp.concatenate([ends, inner.astype(jnp.int32)])
    order = jax.random.permutation(jax.random.fold_in(key, 13), KEPT)
    return whole[order].astype(jnp.int32)


def place_ends(values, rng, least, largest):
    place = [jax.random.randint(jax.random.fold_in(rng, axis), (), 0, length) for axis, length in enumerate(values.shape)]
    main_axis = values.shape.index(max(values.shape))
    next_to = place[:main_axis] + [(place[main_axis] + 1) % values.shape[main_axis]] + place[main_axis + 1:]
    return values.at[tuple(place)].set(least).at[tuple(next_to)].set(largest)


def steps_of(stream_key, shape, pieces, low, top_value):
    level = 1.0
    for dim, blocks in pieces:
        steps = jax.random.uniform(jax.random.fold_in(jax.random.fold_in(stream_key, 6), dim), (blocks,), jnp.float32, low / len(pieces), top_value / len(pieces))
        level = level * jnp.repeat(jnp.exp(steps), shape[dim] // blocks).reshape((-1,) + (1,) * (len(shape) - 1 - dim))
    return level


def normal_values(key, shape, spread, bound, cuts=(), kind=jnp.bfloat16):
    result = jax.random.normal(key, shape, jnp.float32) * spread
    if len(cuts) > 0:
        result = steps_of(key, shape, cuts, -0.22, 0.18) * result
    return jnp.clip(result, min=-bound, max=bound).astype(kind)


def setup_inputs(seed: int = 0) -> dict:
    seeds = jax.random.split(jax.random.key(seed), 10)
    beam_states = normal_values(seeds[0], (BEAMS, D), 1.0, 6.0, ((0, 8), (1, 4)))
    step_tokens = normal_values(seeds[1], (STEPS, BEAMS, D), 1.0, 6.0, ((1, 8), (2, 4)))
    norm_gain = jnp.clip(1.0 + 0.15 * jax.random.normal(seeds[2], (D,), jnp.float32), 0.25, 1.75).astype(jnp.bfloat16)
    w_gate = normal_values(seeds[3], (D, FF), D ** -0.5, 0.046875, ((0, 4), (1, 8)))
    w_up = normal_values(seeds[4], (D, FF), D ** -0.5, 0.046875, ((0, 4), (1, 8)))
    w_down = normal_values(seeds[5], (FF, D), FF ** -0.5, 0.03125, ((0, 8), (1, 4)))
    prompt_table = normal_values(seeds[6], (PTOK, D), 1.0, 6.0, ((1, 4),))
    kept_beams = draw_kept_beams(jax.random.fold_in(seeds[9], 71), 0)
    prompt_ids = place_ends(jax.random.randint(seeds[8], (KEPT, PROMPT), 0, PTOK), jax.random.fold_in(seeds[8], 1), 0, PTOK - 1).astype(jnp.int32)
    return {"beam_states": beam_states, "step_tokens": step_tokens, "norm_gain": norm_gain, "w_gate": w_gate, "w_up": w_up, "w_down": w_down, "prompt_table": prompt_table, "kept_beams": kept_beams, "prompt_ids": prompt_ids}


EPS = 1e-05

def layer(rows, norm_gain, w_gate, w_up, w_down):
    values = rows.astype(jnp.float32)
    scale = lax.rsqrt(lax.optimization_barrier(jnp.sum(values * values, axis=1, keepdims=True)) / D + EPS)
    scaled = (values * norm_gain.astype(jnp.float32)).astype(jnp.bfloat16)
    gate = scale * jnp.dot(scaled, w_gate, preferred_element_type=jnp.float32)
    upper = scale * jnp.dot(scaled, w_up, preferred_element_type=jnp.float32)
    hidden = (jax.nn.silu(gate) * upper).astype(jnp.bfloat16)
    return jnp.dot(hidden, w_down, preferred_element_type=jnp.float32)

def reference(beam_states, step_tokens, norm_gain, w_gate, w_up, w_down, prompt_table, kept_beams, prompt_ids):
    state = beam_states
    for step in range(STEPS):
        mixed = (state.astype(jnp.float32) + step_tokens[step].astype(jnp.float32)).astype(jnp.bfloat16)
        state = (mixed.astype(jnp.float32) + layer(mixed, norm_gain, w_gate, w_up, w_down)).astype(jnp.bfloat16)
    chosen = state[kept_beams].astype(jnp.float32)
    words = prompt_table[prompt_ids].astype(jnp.float32)
    rows = (chosen[:, None, :] + words).astype(jnp.bfloat16).reshape(KEPT * PROMPT, D)
    evaluated = (rows.astype(jnp.float32) + layer(rows, norm_gain, w_gate, w_up, w_down)).astype(jnp.bfloat16)
    return (state, evaluated)
```

```python
import functools

import jax
import jax.numpy as jnp
from jax import lax
from jax.experimental import pallas as pl
from jax.experimental.pallas import tpu as pltpu
from jax.sharding import PartitionSpec as P

EPS = 1e-05
BF = jnp.bfloat16
F32 = jnp.float32
DEPTH = 6
VMEM_LIMIT = 48 * 2**20


def dot(a, b):
    return jnp.dot(a, b, preferred_element_type=F32)


def block_of(width):
    return 256 if width % 256 == 0 else 128


def aligned(start, size):
    return pl.ds(pl.multiple_of(start, 128), size)


def pick_rows(source, count):
    column = lax.broadcasted_iota(jnp.int32, (source.shape[0], count), 1)
    return (column == source).astype(BF)


def stream(copies_of, count, use):
    for n in range(min(DEPTH, count)):
        for copy in copies_of(n, n):
            copy.start()
    yield

    def body(n, carry):
        slot = lax.rem(n, DEPTH)
        for copy in copies_of(n, slot):
            copy.wait()
        use(n, slot)

        @pl.when(n + DEPTH < count)
        def _():
            for copy in copies_of(n + DEPTH, slot):
                copy.start()

        return carry

    lax.fori_loop(0, count, body, 0)


def up_kernel(groups, block, where_ref, xa_ref, xb_ref, gain_ref, wg_ref, wu_ref, own_ref, *rest):
    messages, (xs_ref, buffers, sems) = rest[:-3], rest[-3:]
    rows, width = xs_ref.shape
    units = wg_ref.shape[1]
    share = rows // groups
    half = width // 2

    def copies_of(n, slot):
        return [
            pltpu.make_async_copy(
                w_ref.at[:, aligned(n * block, block)], buffers.at[slot, part], sems.at[slot, part]
            )
            for part, w_ref in enumerate((wg_ref, wu_ref))
        ]

    def use(n, slot):
        columns = aligned(n * block, block)
        for part in range(2):
            value = dot(xs_ref[...], buffers[slot, part])
            own_ref[part, :, columns] = value[:share]
            for j, message in enumerate(messages, 1):
                message[part, :, columns] = value[j * share : (j + 1) * share].astype(BF)

    streaming = stream(copies_of, units // block, use)
    next(streaming)

    a = xa_ref[...].astype(F32)
    b = xb_ref[...].astype(F32)
    swap = where_ref[1] == 1
    low = jnp.where(swap, b, a)
    high = jnp.where(swap, a, b)
    squares = jnp.sum(low * low, axis=1, keepdims=True) + jnp.sum(high * high, axis=1, keepdims=True)
    squares = jnp.broadcast_to(squares, (rows, 128))
    place = lax.broadcasted_iota(jnp.int32, (rows, 1), 0)
    slab = jnp.bitwise_xor(place // share, where_ref[0])
    picker = pick_rows(slab * share + place % share, rows)
    gain = gain_ref[...].astype(F32)
    xs_ref[:, :half] = dot(picker, (low * gain[:, :half]).astype(BF)).astype(BF)
    xs_ref[:, half:] = dot(picker, (high * gain[:, half:]).astype(BF)).astype(BF)
    top = squares.astype(BF)
    for part, piece in enumerate((top, (squares - top.astype(F32)).astype(BF))):
        value = dot(picker, piece)
        own_ref[part, :, units:] = value[:share]
        for j, message in enumerate(messages, 1):
            message[part, :, units:] = value[j * share : (j + 1) * share].astype(BF)

    for _ in streaming:
        pass


def up_project(where, xa, xb, gain, w_gate, w_up, groups):
    rows = xa.shape[0]
    width, units = w_gate.shape
    block = block_of(units)
    shape = (2, rows // groups, units + 128)
    vmem = pl.BlockSpec(memory_space=pltpu.VMEM)
    anywhere = pl.BlockSpec(memory_space=pl.ANY)
    return pl.pallas_call(
        functools.partial(up_kernel, groups, block),
        in_specs=[pl.BlockSpec(memory_space=pltpu.SMEM), vmem, vmem, vmem, anywhere, anywhere],
        out_specs=[vmem] * groups,
        scratch_shapes=[
            pltpu.VMEM((rows, width), BF),
            pltpu.VMEM((DEPTH, 2, width, block), BF),
            pltpu.SemaphoreType.DMA((DEPTH, 2)),
        ],
        out_shape=[jax.ShapeDtypeStruct(shape, F32)] + [jax.ShapeDtypeStruct(shape, BF)] * (groups - 1),
        compiler_params=pltpu.CompilerParams(vmem_limit_bytes=VMEM_LIMIT),
        cost_estimate=pl.CostEstimate(
            flops=4 * rows * width * units, bytes_accessed=4 * width * units, transcendentals=0
        ),
        name="up_project",
    )(where, xa, xb, gain, w_gate, w_up)


def down_kernel(groups, source_of, by_columns, block, where_ref, *rest):
    slabs, w_ref, keep_ref, send_ref = rest[:groups], rest[groups], rest[groups + 1], rest[groups + 2]
    hs_ref, buffers, sems = rest[-3:]
    rows, share = hs_ref.shape[0], slabs[0].shape[0]
    columns = w_ref.shape[1]
    half = columns // 2

    def copies_of(n, slot):
        start = n * block
        if by_columns:
            late = start >= half
            side = jnp.where(late, where_ref[1], 1 - where_ref[1])
            start = side * half + jnp.where(late, start - half, start)
        return [
            pltpu.make_async_copy(w_ref.at[:, aligned(start, block)], buffers.at[slot], sems.at[slot])
        ]

    def use(n, slot):
        value = dot(hs_ref[...], buffers[slot])
        start = n * block
        if by_columns:

            @pl.when(start < half)
            def _():
                send_ref[:, aligned(start, block)] = value.astype(BF)

            @pl.when(start >= half)
            def _():
                keep_ref[:, aligned(start - half, block)] = value

        else:
            keep_ref[:, aligned(start, block)] = value[: rows // 2]
            send_ref[:, aligned(start, block)] = value[rows // 2 :].astype(BF)

    streaming = stream(copies_of, columns // block, use)
    next(streaming)
    source = source_of(where_ref, lax.broadcasted_iota(jnp.int32, (rows, 1), 0))
    slab = jnp.bitwise_xor(source // share, where_ref[0])
    total = 0.0
    for j, slab_ref in enumerate(slabs):
        local = jnp.where(slab == j, source % share, -1)
        total = total + dot(pick_rows(local, share), slab_ref[...])
    hs_ref[...] = total.astype(BF)
    for _ in streaming:
        pass


def down_project(where, slabs, w_down, source_of, by_columns):
    groups = len(slabs)
    rows = groups * slabs[0].shape[0]
    units, columns = w_down.shape
    block = block_of(columns // 2)
    shape = (rows, columns // 2) if by_columns else (rows // 2, columns)
    vmem = pl.BlockSpec(memory_space=pltpu.VMEM)
    return pl.pallas_call(
        functools.partial(down_kernel, groups, source_of, by_columns, block),
        in_specs=[pl.BlockSpec(memory_space=pltpu.SMEM)]
        + [vmem] * groups
        + [pl.BlockSpec(memory_space=pl.ANY)],
        out_specs=[vmem, vmem],
        scratch_shapes=[
            pltpu.VMEM((rows, units), BF),
            pltpu.VMEM((DEPTH, units, block), BF),
            pltpu.SemaphoreType.DMA((DEPTH,)),
        ],
        out_shape=[jax.ShapeDtypeStruct(shape, F32), jax.ShapeDtypeStruct(shape, BF)],
        compiler_params=pltpu.CompilerParams(vmem_limit_bytes=VMEM_LIMIT),
        cost_estimate=pl.CostEstimate(
            flops=2 * rows * units * columns, bytes_accessed=2 * units * columns, transcendentals=0
        ),
        name="down_project",
    )(where, *slabs, w_down)


def far_first(count):
    return sorted(range(1, count), key=lambda k: -k)


def on_device(
    beam_states, step_tokens, norm_gain, w_gate, w_up, w_down, prompt_table, kept_beams, prompt_ids
):
    gx, gy = lax.axis_size("gx"), lax.axis_size("gy")
    chips = gy // 2
    me = lax.axis_index("gx")
    mine = lax.axis_index("gy")
    core, chip = mine % 2, mine // 2
    steps, share, width = step_tokens.shape
    model = width * gx
    units = w_gate.shape[1]
    half = width // 2
    gain = norm_gain.reshape(1, width)

    def swap_gx(x, k):
        return lax.ppermute(x, "gx", [(i, i ^ k) for i in range(gx)])

    def swap_gy(x, k):
        return lax.ppermute(x, "gy", [(i, i ^ k) for i in range(gy)])

    def in_order(own, other):
        return jnp.where(core == 0, own, other), jnp.where(core == 0, other, own)

    def hidden_slabs(xa, xb, swap):
        where = jnp.stack([me, swap]).astype(jnp.int32)
        own, *messages = up_project(where, xa, xb, gain, w_gate, w_up, gx)
        arrived = {k: swap_gx(messages[k - 1], k) for k in far_first(gx)}
        total = own
        for k in range(1, gx):
            total = total + arrived[k].astype(F32)
        squares = total[0, :, units] + total[1, :, units]
        scale = lax.rsqrt(squares / model + EPS)[:, None]
        gate, upper = total[0, :, :units], total[1, :, :units]
        hidden = (jax.nn.silu(scale * gate) * (scale * upper)).astype(BF)
        arrived = {k: swap_gx(hidden, k) for k in far_first(gx)}
        return [hidden] + [arrived[k] for k in range(1, gx)]

    def half_columns(x):
        return (
            lax.dynamic_slice_in_dim(x, core * half, half, x.ndim - 1),
            lax.dynamic_slice_in_dim(x, (1 - core) * half, half, x.ndim - 1),
        )

    first = (beam_states.astype(F32) + step_tokens[0].astype(F32)).astype(BF)
    pieces = jnp.concatenate([first[None], step_tokens[1:]])
    own_half, other_half = half_columns(pieces)
    both = jnp.concatenate(in_order(own_half, swap_gy(other_half, 1)), axis=1)
    arrived = {k: swap_gy(both, 2 * k) for k in far_first(chips)}
    slabs = jnp.stack([both] + [arrived[k] for k in range(1, chips)])
    ordered = [lax.dynamic_index_in_dim(slabs, jnp.bitwise_xor(chip, z), 0, False) for z in range(chips)]
    gathered = jnp.concatenate(ordered, axis=1)

    mixed = gathered[0]
    for step in range(steps):
        partner = swap_gy(mixed, 1)
        slabs = hidden_slabs(mixed, partner, core)
        where = jnp.stack([me, core]).astype(jnp.int32)
        straight = lambda s, place: place
        keep, send = down_project(where, slabs, w_down, straight, True)
        total = keep + swap_gy(send, 1).astype(F32)
        span = 1
        while span < chips:
            rounded = total.astype(BF)
            total = rounded.astype(F32) + swap_gy(rounded, 2 * (2 * span - 1)).astype(F32)
            span *= 2
        state = (mixed.astype(F32) + total).astype(BF)
        if step + 1 < steps:
            mixed = (state.astype(F32) + gathered[step + 1].astype(F32)).astype(BF)

    every_beam = jnp.concatenate(in_order(state, swap_gy(state, 1)), axis=1)
    decoded = lax.dynamic_slice_in_dim(every_beam, mine * share, share, 0)

    beam_index = lax.iota(jnp.int32, every_beam.shape[0])
    picker = (kept_beams[:, None] == beam_index[None, :]).astype(BF)
    chosen = dot(picker, every_beam)
    token_index = lax.iota(jnp.int32, prompt_table.shape[0])
    lookup = (prompt_ids.reshape(-1)[:, None] == token_index[None, :]).astype(BF)
    words = dot(lookup, prompt_table)
    rows = (jnp.repeat(chosen, prompt_ids.shape[1], axis=0) + words).astype(BF)

    count = rows.shape[0] // gy
    own_rows = lax.dynamic_slice_in_dim(rows, mine * count, count, 0)
    slabs = hidden_slabs(rows[:, :half], rows[:, half:], jnp.int32(0))

    def by_owner(s, place):
        owner_core = jnp.bitwise_xor(place // (chips * count), s[1])
        owner_chip = jnp.bitwise_xor(place // count % chips, s[2])
        return (owner_chip * 2 + owner_core) * count + place % count

    where = jnp.stack([me, core, chip]).astype(jnp.int32)
    keep, send = down_project(where, slabs, w_down, by_owner, False)
    total = (keep + swap_gy(send, 1).astype(F32)).reshape(chips, count, width)
    rounded = total.astype(BF)
    arrived = {k: swap_gy(rounded[k], 2 * k) for k in far_first(chips)}
    result = own_rows.astype(F32) + total[0]
    for k in range(1, chips):
        result = result + arrived[k].astype(F32)
    return (decoded, result.astype(BF))


def solution(mesh):
    return jax.shard_map(
        on_device,
        mesh=mesh,
        in_specs=(
            P("gy", "gx"),
            P(None, "gy", "gx"),
            P("gx"),
            P("gx", "gy"),
            P("gx", "gy"),
            P("gy", "gx"),
            P(None, "gx"),
            P(),
            P(),
        ),
        out_specs=(P("gy", "gx"), P("gy", "gx")),
        check_vma=False,
    )
```

```python
import functools

import jax
import jax.numpy as jnp
from jax import lax
from jax.experimental import pallas as pl
from jax.experimental.pallas import tpu as pltpu
from jax.sharding import PartitionSpec as P


EPS = 1e-05
BF = jnp.bfloat16
F32 = jnp.float32
DEPTH = 6
VMEM_LIMIT = 48 * 2**20


def dot(a, b):
    return jnp.dot(a, b, preferred_element_type=F32)


def block_of(width):
    return 256 if width % 256 == 0 else 128


def aligned(start, size):
    return pl.ds(pl.multiple_of(start, 128), size)


def pick_rows(source, count):
    column = lax.broadcasted_iota(jnp.int32, (source.shape[0], count), 1)
    return (column == source).astype(BF)


def stream(copies_of, count, use):
    for n in range(min(DEPTH, count)):
        for copy in copies_of(n, n):
            copy.start()
    yield

    def body(n, carry):
        slot = lax.rem(n, DEPTH)
        for copy in copies_of(n, slot):
            copy.wait()
        use(n, slot)

        @pl.when(n + DEPTH < count)
        def _():
            for copy in copies_of(n + DEPTH, slot):
                copy.start()

        return carry

    lax.fori_loop(0, count, body, 0)


def up_kernel(groups, block, first, where_ref, xa_ref, xb_ref, gain_ref, wg_ref, wu_ref, own_ref, *rest):
    messages, (xs_ref, buffers, sems) = rest[:-3], rest[-3:]
    rows, width = xs_ref.shape
    units = own_ref.shape[2] // block * block
    share = rows // groups
    half = width // 2

    def copies_of(n, slot):
        return [
            pltpu.make_async_copy(
                w_ref.at[:, aligned(first + n * block, block)], buffers.at[slot, part], sems.at[slot, part]
            )
            for part, w_ref in enumerate((wg_ref, wu_ref))
        ]

    def use(n, slot):
        columns = aligned(n * block, block)
        for part in range(2):
            value = dot(xs_ref[...], buffers[slot, part])
            own_ref[part, :, columns] = value[:share]
            for j, message in enumerate(messages, 1):
                message[part, :, columns] = value[j * share : (j + 1) * share].astype(BF)

    streaming = stream(copies_of, units // block, use)
    next(streaming)

    a = xa_ref[...].astype(F32)
    b = xb_ref[...].astype(F32)
    swap = where_ref[1] == 1
    low = jnp.where(swap, b, a)
    high = jnp.where(swap, a, b)
    squares = jnp.sum(low * low, axis=1, keepdims=True) + jnp.sum(high * high, axis=1, keepdims=True)
    squares = jnp.broadcast_to(squares, (rows, 128))
    place = lax.broadcasted_iota(jnp.int32, (rows, 1), 0)
    slab = jnp.bitwise_xor(place // share, where_ref[0])
    picker = pick_rows(slab * share + place % share, rows)
    gain = gain_ref[...].astype(F32)
    xs_ref[:, :half] = dot(picker, (low * gain[:, :half]).astype(BF)).astype(BF)
    xs_ref[:, half:] = dot(picker, (high * gain[:, half:]).astype(BF)).astype(BF)
    if units < own_ref.shape[2]:
        top = squares.astype(BF)
        for part, piece in enumerate((top, (squares - top.astype(F32)).astype(BF))):
            value = dot(picker, piece)
            own_ref[part, :, units:] = value[:share]
            for j, message in enumerate(messages, 1):
                message[part, :, units:] = value[j * share : (j + 1) * share].astype(BF)

    for _ in streaming:
        pass


def up_project(where, xa, xb, gain, w_gate, w_up, groups, first, units):
    rows = xa.shape[0]
    width = w_gate.shape[0]
    block = block_of(w_gate.shape[1])
    shape = (2, rows // groups, units + (128 if first == 0 else 0))
    vmem = pl.BlockSpec(memory_space=pltpu.VMEM)
    anywhere = pl.BlockSpec(memory_space=pl.ANY)
    return pl.pallas_call(
        functools.partial(up_kernel, groups, block, first),
        in_specs=[pl.BlockSpec(memory_space=pltpu.SMEM), vmem, vmem, vmem, anywhere, anywhere],
        out_specs=[vmem] * groups,
        scratch_shapes=[
            pltpu.VMEM((rows, width), BF),
            pltpu.VMEM((DEPTH, 2, width, block), BF),
            pltpu.SemaphoreType.DMA((DEPTH, 2)),
        ],
        out_shape=[jax.ShapeDtypeStruct(shape, F32)] + [jax.ShapeDtypeStruct(shape, BF)] * (groups - 1),
        compiler_params=pltpu.CompilerParams(vmem_limit_bytes=VMEM_LIMIT),
        cost_estimate=pl.CostEstimate(
            flops=4 * rows * width * units, bytes_accessed=4 * width * units, transcendentals=0
        ),
        name="up_project",
    )(where, xa, xb, gain, w_gate, w_up)


def down_kernel(groups, source_of, by_columns, block, where_ref, *rest):
    slabs, w_ref, keep_ref, send_ref = rest[:groups], rest[groups], rest[groups + 1], rest[groups + 2]
    hs_ref, buffers, sems = rest[-3:]
    rows, share = hs_ref.shape[0], slabs[0].shape[0]
    columns = w_ref.shape[1]
    half = columns // 2

    def copies_of(n, slot):
        start = n * block
        if by_columns:
            late = start >= half
            side = jnp.where(late, where_ref[1], 1 - where_ref[1])
            start = side * half + jnp.where(late, start - half, start)
        return [
            pltpu.make_async_copy(w_ref.at[:, aligned(start, block)], buffers.at[slot], sems.at[slot])
        ]

    def use(n, slot):
        value = dot(hs_ref[...], buffers[slot])
        start = n * block
        if by_columns:

            @pl.when(start < half)
            def _():
                send_ref[:, aligned(start, block)] = value.astype(BF)

            @pl.when(start >= half)
            def _():
                keep_ref[:, aligned(start - half, block)] = value

        else:
            keep_ref[:, aligned(start, block)] = value[: rows // 2]
            send_ref[:, aligned(start, block)] = value[rows // 2 :].astype(BF)

    streaming = stream(copies_of, columns // block, use)
    next(streaming)
    source = source_of(where_ref, lax.broadcasted_iota(jnp.int32, (rows, 1), 0))
    slab = jnp.bitwise_xor(source // share, where_ref[0])
    total = 0.0
    for j, slab_ref in enumerate(slabs):
        local = jnp.where(slab == j, source % share, -1)
        total = total + dot(pick_rows(local, share), slab_ref[...])
    hs_ref[...] = total.astype(BF)
    for _ in streaming:
        pass


def down_project(where, slabs, w_down, source_of, by_columns):
    groups = len(slabs)
    rows = groups * slabs[0].shape[0]
    units, columns = w_down.shape
    block = block_of(columns // 2)
    shape = (rows, columns // 2) if by_columns else (rows // 2, columns)
    vmem = pl.BlockSpec(memory_space=pltpu.VMEM)
    return pl.pallas_call(
        functools.partial(down_kernel, groups, source_of, by_columns, block),
        in_specs=[pl.BlockSpec(memory_space=pltpu.SMEM)]
        + [vmem] * groups
        + [pl.BlockSpec(memory_space=pl.ANY)],
        out_specs=[vmem, vmem],
        scratch_shapes=[
            pltpu.VMEM((rows, units), BF),
            pltpu.VMEM((DEPTH, units, block), BF),
            pltpu.SemaphoreType.DMA((DEPTH,)),
        ],
        out_shape=[jax.ShapeDtypeStruct(shape, F32), jax.ShapeDtypeStruct(shape, BF)],
        compiler_params=pltpu.CompilerParams(vmem_limit_bytes=VMEM_LIMIT),
        cost_estimate=pl.CostEstimate(
            flops=2 * rows * units * columns, bytes_accessed=2 * units * columns, transcendentals=0
        ),
        name="down_project",
    )(where, *slabs, w_down)


def far_first(count):
    return sorted(range(1, count), key=lambda k: -k)


def on_device(
    beam_states, step_tokens, norm_gain, w_gate, w_up, w_down, prompt_table, kept_beams, prompt_ids
):
    gx, gy = lax.axis_size("gx"), lax.axis_size("gy")
    chips = gy // 2
    me = lax.axis_index("gx")
    mine = lax.axis_index("gy")
    core, chip = mine % 2, mine // 2
    steps, share, width = step_tokens.shape
    model = width * gx
    units = w_gate.shape[1]
    half = width // 2
    gain = norm_gain.reshape(1, width)
    block = block_of(units)
    cut = -(-units // block * 4 // 7) * block

    def swap_gx(x, k):
        return lax.ppermute(x, "gx", [(i, i ^ k) for i in range(gx)])

    def swap_gy(x, k):
        return lax.ppermute(x, "gy", [(i, i ^ k) for i in range(gy)])

    def in_order(own, other):
        return jnp.where(core == 0, own, other), jnp.where(core == 0, other, own)

    def hidden_slabs(xa, xb, swap, cuts):
        where = jnp.stack([me, swap]).astype(jnp.int32)
        sums, scale = [], None
        for first, last in zip(cuts, cuts[1:]):
            own, *messages = up_project(where, xa, xb, gain, w_gate, w_up, gx, first, last - first)
            arrived = {}
            for k in far_first(gx):
                arrived[k] = swap_gx(messages[k - 1], k)
            sums.append((own, arrived))
        pieces = []
        for (own, arrived), first, last in zip(sums, cuts, cuts[1:]):
            count = last - first
            total = own
            for k in range(1, gx):
                total = total + arrived[k].astype(F32)
            if first == 0:
                squares = total[0, :, count] + total[1, :, count]
                scale = lax.rsqrt(squares / model + EPS)[:, None]
            gate, upper = total[0, :, :count], total[1, :, :count]
            pieces.append((jax.nn.silu(scale * gate) * (scale * upper)).astype(BF))
        hidden = jnp.concatenate(pieces, axis=1)
        arrived = {k: swap_gx(hidden, k) for k in far_first(gx)}
        return [hidden] + [arrived[k] for k in range(1, gx)]

    def half_columns(x):
        return (
            lax.dynamic_slice_in_dim(x, core * half, half, x.ndim - 1),
            lax.dynamic_slice_in_dim(x, (1 - core) * half, half, x.ndim - 1),
        )

    first = (beam_states.astype(F32) + step_tokens[0].astype(F32)).astype(BF)
    pieces = jnp.concatenate([first[None], step_tokens[1:]])
    own_half, other_half = half_columns(pieces)
    both = jnp.concatenate(in_order(own_half, swap_gy(other_half, 1)), axis=1)
    arrived = {k: swap_gy(both, 2 * k) for k in far_first(chips)}
    slabs = jnp.stack([both] + [arrived[k] for k in range(1, chips)])
    ordered = [lax.dynamic_index_in_dim(slabs, jnp.bitwise_xor(chip, z), 0, False) for z in range(chips)]
    gathered = jnp.concatenate(ordered, axis=1)

    mixed = gathered[0]
    for step in range(steps):
        partner = swap_gy(mixed, 1)
        slabs = hidden_slabs(mixed, partner, core, (0, units))
        where = jnp.stack([me, core]).astype(jnp.int32)
        straight = lambda s, place: place
        keep, send = down_project(where, slabs, w_down, straight, True)
        total = keep + swap_gy(send, 1).astype(F32)
        span = 1
        while span < chips:
            rounded = total.astype(BF)
            total = rounded.astype(F32) + swap_gy(rounded, 2 * (2 * span - 1)).astype(F32)
            span *= 2
        state = (mixed.astype(F32) + total).astype(BF)
        if step + 1 < steps:
            mixed = (state.astype(F32) + gathered[step + 1].astype(F32)).astype(BF)

    every_beam = jnp.concatenate(in_order(state, swap_gy(state, 1)), axis=1)
    decoded = lax.dynamic_slice_in_dim(every_beam, mine * share, share, 0)

    beam_index = lax.iota(jnp.int32, every_beam.shape[0])
    picker = (kept_beams[:, None] == beam_index[None, :]).astype(BF)
    chosen = dot(picker, every_beam)
    token_index = lax.iota(jnp.int32, prompt_table.shape[0])
    lookup = (prompt_ids.reshape(-1)[:, None] == token_index[None, :]).astype(BF)
    words = dot(lookup, prompt_table)
    rows = (jnp.repeat(chosen, prompt_ids.shape[1], axis=0) + words).astype(BF)

    count = rows.shape[0] // gy
    own_rows = lax.dynamic_slice_in_dim(rows, mine * count, count, 0)
    slabs = hidden_slabs(rows[:, :half], rows[:, half:], jnp.int32(0), (0, cut, units))

    def by_owner(s, place):
        owner_core = jnp.bitwise_xor(place // (chips * count), s[1])
        owner_chip = jnp.bitwise_xor(place // count % chips, s[2])
        return (owner_chip * 2 + owner_core) * count + place % count

    where = jnp.stack([me, core, chip]).astype(jnp.int32)
    keep, send = down_project(where, slabs, w_down, by_owner, False)
    total = (keep + swap_gy(send, 1).astype(F32)).reshape(chips, count, width)
    rounded = total.astype(BF)
    arrived = {k: swap_gy(rounded[k], 2 * k) for k in far_first(chips)}
    result = own_rows.astype(F32) + total[0]
    for k in range(1, chips):
        result = result + arrived[k].astype(F32)
    return (decoded, result.astype(BF))


def solution(mesh):
    return jax.shard_map(
        on_device,
        mesh=mesh,
        in_specs=(
            P("gy", "gx"),
            P(None, "gy", "gx"),
            P("gx"),
            P("gx", "gy"),
            P("gx", "gy"),
            P("gy", "gx"),
            P(None, "gx"),
            P(),
            P(),
        ),
        out_specs=(P("gy", "gx"), P("gy", "gx")),
        check_vma=False,
    )
```
